256 devices in a mesh: groups: 4 (over y, x), tp: 32 (over z), sp: 2 (over core).
Axes of the slice: x: 2, y: 2, z: 32, core: 2. Of those that a mesh axis runs over, the one named last changes fastest.
The devices are a block of a 4x8x32 slice.
Arguments:
- tokens: bfloat16 [12288, 4608], P(('groups', 'tp', 'sp')), parts along dimension 0, may hold values from -48 to 48
- w_query: bfloat16 [4608, 4096], P(None, 'tp'), may hold values from -0.09375 to 0.09375
- w_key: bfloat16 [4608, 2048], P(None, 'tp'), may hold values from -0.09375 to 0.09375
- w_value: bfloat16 [4608, 2048], P(None, 'tp'), may hold values from -0.09375 to 0.09375
- w_out: bfloat16 [4096, 4608], P('tp'), may hold values from -0.5 to 0.5
- doc_lengths: int32 [32], P('groups'), parts along dimension 0, may hold values from 1 to 768, 3072 in all
Outputs:
- attn_out: bfloat16 [12288, 4608], P(('groups', 'tp', 'sp')), parts along dimension 0
The draws below stay inside these ranges and needn't reach their ends.
There are 4 independent parts, one for each index of `groups`. The reference program is written for one: setup_inputs(seed, part) draws one part's arguments, and reference() takes and returns one part's arrays. A program takes and returns all parts, laid end to end along the dimension named above; an argument that names none is the same for every part. Nothing has to cross between parts.
Inputs may be any that keep to these rules, and one draw needn't show every extreme that they name: `doc_lengths`: positive lengths that sum to 3072; the largest is exactly a quarter of 3072.
All inputs are finite; a program needn't handle non-finite values.
Results may differ from the reference program's by a relative error of at most 0.024.
Values may be sent and summed in bfloat16 or wider, within the bound.
A program may use at most 128 MiB of HBM per device.

```python
import math
import jax
import jax.numpy as jnp
import numpy as np
from jax import lax

D = 4608
HD = 128
PRE_SCALE = 144
DOCS = 8
HEADS = 32
KV_HEADS = 16
SEQ = 3072


def draw_tokens(key, part):
    normal_key = jax.random.fold_in(jax.random.fold_in(key, 11), 0)
    base_draw = jnp.clip(jax.random.normal(normal_key, (SEQ, D), jnp.float32), -6.0, 6.0)
    return base_draw.astype(jnp.bfloat16)


def steps_of(key, dims, shards, smallest, top_value):
    gain = 1.0
    for dim, blocks in shards:
        draws = jax.random.uniform(jax.random.fold_in(jax.random.fold_in(key, 6), dim), (blocks,), jnp.float32, smallest / len(shards), top_value / len(shards))
        gain = gain * jnp.repeat(jnp.exp(draws), dims[dim] // blocks).reshape((-1,) + (1,) * (len(dims) - 1 - dim))
    return gain


def profile(count, total, reach, slope):
    loads = [(1 << 20) // math.isqrt(rank ** slope) + 1 for rank in range(2, count + 1)]
    rest, given = total - reach - (count - 1), [1] * (count - 1)
    while rest > 0:
        candidates = [i for i in range(count - 1) if given[i] < reach]
        pool, budget = sum([loads[i] for i in candidates]), rest
        for i in candidates:
            more = min(reach - given[i], max(1, budget * loads[i] // pool), rest)
            given[i] = given[i] + more
            rest = rest - more
    return np.array([reach] + given)


def ragged(rng, amount, total, limit, skew):
    if amount == 2:
        one = jax.random.randint(rng, (), max(1, total - limit), min(limit, total - 1) + 1)
        return jnp.stack([one, total - one])
    sizes = jnp.asarray(profile(amount, total, limit, skew), jnp.int32)
    twos = (amount - 1) // 2
    source_of, sink = sizes[1:1 + 2 * twos:2], sizes[2:2 + 2 * twos:2]
    margin = jnp.minimum(source_of - 1, limit - sink)
    shifted = jax.random.randint(jax.random.fold_in(rng, 1), (twos,), 0, 1 << 20) % (margin + 1)
    sizes = sizes.at[1:1 + 2 * twos:2].set(source_of - shifted).at[2:2 + 2 * twos:2].set(sink + shifted)
    return sizes[jax.random.permutation(jax.random.fold_in(rng, 2), amount)]


def noise(own_key, shape, deviation, bound, cuts=(), held_as=jnp.bfloat16):
    result = deviation * jax.random.normal(own_key, shape, jnp.float32)
    if cuts:
        result = result * steps_of(own_key, shape, cuts, -0.22, 0.18)
    return jnp.clip(result, -bound, bound).astype(held_as)


def setup_inputs(seed: int = 0, part: int = 0) -> dict:
    key_list = jax.random.split(jax.random.key(seed), 7)
    part_splits = jax.random.split(jax.random.fold_in(key_list[6], part), 7)
    return {
        "tokens": draw_tokens(jax.random.fold_in(jax.random.fold_in(key_list[6], part), 71), part),
        "w_query": noise(key_list[1], (D, HEADS * HD), D ** -0.5, 0.09375, ((1, 32),)),
        "w_key": noise(key_list[2], (D, KV_HEADS * HD), D ** -0.5, 0.09375, ((1, 32),)),
        "w_value": noise(key_list[3], (D, KV_HEADS * HD), D ** -0.5, 0.09375, ((1, 32),)),
        "w_out": noise(key_list[4], (HEADS * HD, D), HD ** -0.5, 0.5, ((0, 32),)),
        "doc_lengths": ragged(part_splits[5], DOCS, SEQ, SEQ // 4, 2).astype(jnp.int32),
    }


def rotate(matrix, places):
    half_width = matrix.shape[1] // 2
    spread = jnp.power(10000.0, -(jnp.arange(half_width, dtype=jnp.float32) * (2.0 / matrix.shape[1])))
    angles = places.astype(jnp.float32)[:, None] * spread[None, :]
    cosine = jnp.cos(angles)
    sine_part = jnp.sin(angles)
    lower_part = matrix[:, :half_width]
    upper_part = matrix[:, half_width:]
    return jnp.concatenate([lower_part * cosine - upper_part * sine_part, upper_part * cosine + lower_part * sine_part], axis=1)


def doc_index(places, doc_ends):
    return jnp.sum((places[:, None] >= doc_ends[None, :]).astype(jnp.int32), axis=1)


def reference(tokens, w_query, w_key, w_value, w_out, doc_lengths):
    length = tokens.shape[0]
    places = jnp.arange(length, dtype=jnp.int32)
    doc_ends = jnp.cumsum(doc_lengths).astype(jnp.int32)
    doc_ids = doc_index(places, doc_ends)
    allowed = (doc_ids[:, None] == doc_ids[None, :]) & (places[None, :] <= places[:, None])
    key_raw = lax.optimization_barrier(jnp.dot(tokens, w_key, preferred_element_type=jnp.float32).astype(jnp.bfloat16))
    value_all = jnp.dot(tokens, w_value, preferred_element_type=jnp.float32).astype(jnp.bfloat16)

    def head_step(running_sum, head_index):
        w_head = lax.dynamic_slice_in_dim(w_query, head_index * HD, HD, 1)
        queries = (rotate(jnp.dot(tokens, w_head, preferred_element_type=jnp.float32), places) * PRE_SCALE ** -0.5).astype(jnp.bfloat16)
        pair_index = head_index // 2
        key_part = lax.dynamic_slice_in_dim(key_raw, pair_index * HD, HD, 1).astype(jnp.float32)
        key_rows = rotate(key_part, places).astype(jnp.bfloat16)
        value_rows = lax.dynamic_slice_in_dim(value_all, pair_index * HD, HD, 1)
        scores = jnp.dot(queries, key_rows.T, preferred_element_type=jnp.float32)
        largest = jnp.max(jnp.where(allowed, scores, -1e30), axis=1, keepdims=True)
        weights = jnp.where(allowed, jnp.exp(scores - largest), 0.0)
        denominator = jnp.sum(weights, axis=1, keepdims=True)
        attended = (jnp.dot(weights.astype(jnp.bfloat16), value_rows, preferred_element_type=jnp.float32) / denominator).astype(jnp.bfloat16)
        w_head_out = lax.dynamic_slice_in_dim(w_out, head_index * HD, HD, 0)
        partial_value = lax.optimization_barrier(jnp.dot(attended, w_head_out, preferred_element_type=jnp.float32).astype(jnp.bfloat16))
        return running_sum + partial_value.astype(jnp.float32), None

    initial = jnp.zeros((length, tokens.shape[1]), jnp.float32)
    summed, _ = lax.scan(head_step, initial, jnp.arange(HEADS, dtype=jnp.int32))
    return summed.astype(jnp.bfloat16)
```

```python
import functools
import math

import jax
import jax.numpy as jnp
import numpy as np
from jax import lax
from jax.experimental import pallas as pl
from jax.experimental.pallas import tpu as pltpu
from jax.sharding import PartitionSpec as P

PRE_SCALE = 144
MASKED = -1e30
MESH = pl.DeviceIdType.MESH
CHUNKS = 3


def kernel(
    n, window, x_hbm, wq_hbm, wk_hbm, wv_hbm, wo_hbm, lens_ref, freq_ref, out_ref,
    tok, w_in, wk, wv, wo, cosv, sinv, query, mine, theirs, kv, att, first, acc,
    load_sem, ag_send, ag_recv, pair_send, pair_recv, sp_send, sp_recv, rs_send, rs_recv,
):
    z = lax.axis_index("tp")
    s = lax.axis_index("sp")
    right, left = lax.rem(z + 1, n), lax.rem(z + n - 1, n)
    parity = lax.rem(z, 2)
    pair = z + 1 - 2 * parity
    other = 1 - s
    side = (right, left)
    half = n // 2
    rows, depth = x_hbm.shape
    hd = wq_hbm.shape[1]
    hh = hd // 2
    sub = rows // CHUNKS
    width = depth // CHUNKS

    def block(offset):
        return lax.rem(z + offset + 2 * n, n)

    def load(src, dst, i):
        return pltpu.make_async_copy(src, dst, load_sem.at[i])

    own_load = load(x_hbm, tok.at[z], 0)
    loads = (
        load(wq_hbm, w_in.at[:, pl.ds(0, hd)], 1),
        load(wk_hbm, wk, 2),
        load(wv_hbm, wv, 3),
        load(wo_hbm, wo, 4),
    )

    def gather_copy(d, hop, b, c):
        piece = tok.at[b, pl.ds(c * sub, sub), :]
        return pltpu.make_async_remote_copy(
            src_ref=piece, dst_ref=piece,
            send_sem=ag_send.at[d, hop, c], recv_sem=ag_recv.at[d, hop, c],
            device_id={"tp": side[d]}, device_id_type=MESH,
        )

    def pair_copy(b):
        return pltpu.make_async_remote_copy(
            src_ref=mine.at[b], dst_ref=theirs.at[b],
            send_sem=pair_send.at[b], recv_sem=pair_recv.at[b],
            device_id={"tp": pair}, device_id_type=MESH,
        )

    def core_copy(b, core):
        piece = kv.at[pl.ds(pl.multiple_of((2 * b + core) * rows, 16), rows), :]
        return pltpu.make_async_remote_copy(
            src_ref=piece, dst_ref=piece,
            send_sem=sp_send.at[b], recv_sem=sp_recv.at[b],
            device_id={"sp": other}, device_id_type=MESH,
        )

    def sum_copy(d, hop, src, c):
        return pltpu.make_async_remote_copy(
            src_ref=src, dst_ref=acc.at[d, hop, c],
            send_sem=rs_send.at[d, hop, c], recv_sem=rs_recv.at[d, hop, c],
            device_id={"tp": side[d]}, device_id_type=MESH,
        )

    lane = lax.broadcasted_iota(jnp.int32, (rows, hd), 1)
    low = lane < hh
    even_mask = (lane * 0 + parity) == 0

    def turn(v, b):
        return v * cosv[b] + pltpu.roll(v, hh, 1) * sinv[b]

    def project(b):
        made = jnp.dot(tok[b], w_in[...], preferred_element_type=jnp.float32)
        places = (2 * b + s) * rows + lax.broadcasted_iota(jnp.int32, (rows, hd), 0)
        angles = places.astype(jnp.float32) * freq_ref[...]
        cosv[b] = jnp.cos(angles)
        sine = jnp.sin(angles)
        sinv[b] = jnp.where(low, -sine, sine)
        query[b] = (turn(made[:, :hd], b) * PRE_SCALE ** (-0.5)).astype(jnp.bfloat16)
        mine[b] = made[:, hd:].astype(jnp.bfloat16)

    def assemble(b):
        pair_copy(b).wait_recv()
        here = mine[b].astype(jnp.float32)
        there = theirs[b].astype(jnp.float32)
        lower = jnp.where(even_mask, here, there)
        upper = jnp.where(even_mask, there, here)
        key_raw = jnp.where(low, lower, pltpu.roll(upper, hh, 1))
        value = jnp.where(low, pltpu.roll(lower, hh, 1), upper)
        at = pl.ds(pl.multiple_of((2 * b + s) * rows, 16), rows)
        kv[at, pl.ds(0, hd)] = turn(key_raw, b).astype(jnp.bfloat16)
        kv[at, pl.ds(hd, hd)] = value.astype(jnp.bfloat16)

    def attend(b, slot):
        start = pl.multiple_of(jnp.maximum((2 * b + s + 1) * rows - window, 0), 16)
        keys = kv[pl.ds(start, window), pl.ds(0, hd)]
        values = kv[pl.ds(start, window), pl.ds(hd, hd)]
        scores = lax.dot_general(
            query[b], keys, (((1,), (1,)), ((), ())), preferred_element_type=jnp.float32
        )
        place = (2 * b + s) * rows + lax.broadcasted_iota(jnp.int32, (rows, 1), 0)
        opens = jnp.zeros((rows, 1), jnp.int32)
        end = jnp.int32(0)
        for j in range(lens_ref.shape[0]):
            end = end + lens_ref[j]
            opens = jnp.where(place >= end, end, opens)
        key_place = start + lax.broadcasted_iota(jnp.int32, (rows, window), 1)
        allowed = (key_place <= place) & (key_place >= opens)
        masked = jnp.where(allowed, scores, MASKED)
        largest = jnp.max(masked, axis=1, keepdims=True)
        weights = jnp.where(allowed, jnp.exp(masked - largest), 0.0)
        denominator = jnp.sum(weights, axis=1, keepdims=True)
        mixed = jnp.dot(
            weights.astype(jnp.bfloat16), values, preferred_element_type=jnp.float32
        )
        att[slot] = (mixed / denominator).astype(jnp.bfloat16)

    def partial(slot, c):
        return jnp.dot(
            att[slot], wo[:, pl.ds(c * width, width)], preferred_element_type=jnp.float32
        )

    own_load.start()
    for copy in loads:
        copy.start()
    barrier = pltpu.get_barrier_semaphore()
    for where in ({"tp": left}, {"tp": right}, {"sp": other}):
        pl.semaphore_signal(barrier, inc=1, device_id=where, device_id_type=MESH)
    pl.semaphore_wait(barrier, 3)
    own_load.wait()
    for c in range(CHUNKS):
        for d in range(2):
            gather_copy(d, 0, z, c).start()
    for copy in loads:
        copy.wait()
    w_in[:, pl.ds(hd, hd)] = jnp.concatenate([wk[...], wv[...]], axis=1)
    project(z)
    pair_copy(z).start()

    def gather_step(t, _):
        came = (block(-1 - t), block(1 + t))
        for c in range(CHUNKS):
            for d in range(2):
                gather_copy(d, t, came[d], c).wait_recv()

                @pl.when((t < half - 2) | (parity == 1 - d))
                def _():
                    gather_copy(d, t + 1, came[d], c).start()

            if c == 0:

                @pl.when(t == 1)
                def _():
                    assemble(z)
                    core_copy(z, s).start()

                @pl.when(t >= 2)
                def _():
                    for b in (block(1 - t), block(t - 1)):
                        assemble(b)
                        core_copy(b, s).start()

        for b in came:
            project(b)
            pair_copy(b).start()
        return 0

    lax.fori_loop(0, half - 1, gather_step, 0)
    far = block(half)
    late = (block(2 - half), block(half - 2), block(1 - half), block(half - 1), far)
    for b in late[:2]:
        assemble(b)
        core_copy(b, s).start()
    for c in range(CHUNKS):
        for d in range(2):

            @pl.when(parity == d)
            def _():
                gather_copy(d, half - 1, far, c).wait_recv()

    project(far)
    pair_copy(far).start()
    for b in late[2:]:
        assemble(b)
        core_copy(b, s).start()

    def core_arrival(b, _):
        core_copy(b, other).wait_recv()
        return 0

    lax.fori_loop(0, n, core_arrival, 0)

    attend(far, 0)
    for c in range(CHUNKS):
        first[c] = partial(0, c).astype(jnp.bfloat16)
        for d in range(2):

            @pl.when(s == d)
            def _():
                sum_copy(d, 0, first.at[c], c).start()

    attend(block(half - 1), 0)
    attend(block(1 - half), 1)

    def sum_step(t, _):
        for c in range(CHUNKS):
            for d in range(2):
                term = partial(d, c)
                here = acc.at[d, t - 1, c]
                arrives = (t > 1) | (s == d)

                @pl.when(arrives)
                def _():
                    sum_copy(d, t - 1, here, c).wait_recv()
                    here[...] = (here[...].astype(jnp.float32) + term).astype(jnp.bfloat16)

                @pl.when(jnp.logical_not(arrives))
                def _():
                    here[...] = term.astype(jnp.bfloat16)

                sum_copy(d, t, here, c).start()
        attend(block(half - 1 - t), 0)
        attend(block(t + 1 - half), 1)
        return 0

    lax.fori_loop(1, half, sum_step, 0)
    for c in range(CHUNKS):
        term = partial(0, c)
        for d in range(2):
            sum_copy(d, half - 1, acc.at[d, half - 1, c], c).wait_recv()
            term = term + acc[d, half - 1, c].astype(jnp.float32)
        out_ref[:, pl.ds(c * width, width)] = term.astype(jnp.bfloat16)

    def sends_done(t, _):
        for c in range(CHUNKS):
            for d in range(2):

                @pl.when((t < half - 1) | (lax.rem(z + half - 1, 2) == d))
                def _():
                    gather_copy(d, t, z, c).wait_send()

                @pl.when((t > 0) | (s == d))
                def _():
                    sum_copy(d, t, first.at[c], c).wait_send()

        return 0

    lax.fori_loop(0, half, sends_done, 0)

    def block_sends_done(b, _):
        pair_copy(b).wait_send()
        core_copy(b, s).wait_send()
        return 0

    lax.fori_loop(0, n, block_sends_done, 0)


def layer(n, cores, tokens, w_query, w_key, w_value, w_out, doc_lengths):
    rows, depth = tokens.shape
    hd = w_query.shape[1]
    half = n // 2
    total = n * cores * rows
    longest = total // 4
    window = min(-(-(longest + rows) // 128) * 128, total)
    width = depth // CHUNKS
    spread = np.power(
        np.float32(10000.0), -(np.arange(hd // 2, dtype=np.float32) * np.float32(2.0 / hd))
    ).astype(np.float32)
    freq = jnp.asarray(np.concatenate([spread, spread])[None, :])
    anywhere = pl.BlockSpec(memory_space=pl.ANY)
    vmem = pl.BlockSpec(memory_space=pltpu.VMEM)
    bf16, f32, dma = jnp.bfloat16, jnp.float32, pltpu.SemaphoreType.DMA
    return pl.pallas_call(
        functools.partial(kernel, n, window),
        out_shape=jax.ShapeDtypeStruct((rows, depth), bf16),
        in_specs=[anywhere] * 5 + [pl.BlockSpec(memory_space=pltpu.SMEM), vmem],
        out_specs=vmem,
        scratch_shapes=[
            pltpu.VMEM((n, rows, depth), bf16),
            pltpu.VMEM((depth, 2 * hd), bf16),
            pltpu.VMEM((depth, hd // 2), bf16),
            pltpu.VMEM((depth, hd // 2), bf16),
            pltpu.VMEM((hd, depth), bf16),
            pltpu.VMEM((n, rows, hd), f32),
            pltpu.VMEM((n, rows, hd), f32),
            pltpu.VMEM((n, rows, hd), bf16),
            pltpu.VMEM((n, rows, hd), bf16),
            pltpu.VMEM((n, rows, hd), bf16),
            pltpu.VMEM((total, 2 * hd), bf16),
            pltpu.VMEM((2, rows, hd), bf16),
            pltpu.VMEM((CHUNKS, rows, width), bf16),
            pltpu.VMEM((2, half, CHUNKS, rows, width), bf16),
            dma((5,)),
            dma((2, half, CHUNKS)),
            dma((2, half, CHUNKS)),
            dma((n,)),
            dma((n,)),
            dma((n,)),
            dma((n,)),
            dma((2, half, CHUNKS)),
            dma((2, half, CHUNKS)),
        ],
        compiler_params=pltpu.CompilerParams(
            collective_id=0, has_side_effects=True, vmem_limit_bytes=60 * 1024 * 1024
        ),
    )(tokens, w_query, w_key, w_value, w_out, doc_lengths, freq)


def solution(mesh):
    placed = (
        P(("groups", "tp", "sp"), None),
        P(None, "tp"),
        P(None, "tp"),
        P(None, "tp"),
        P("tp", None),
        P("groups"),
    )
    return jax.shard_map(
        functools.partial(layer, mesh.shape["tp"], mesh.shape["sp"]),
        mesh=mesh,
        in_specs=placed,
        out_specs=P(("groups", "tp", "sp"), None),
        check_vma=False,
    )
```

```python
import functools
import math

import jax
import jax.numpy as jnp
import numpy as np
from jax import lax
from jax.experimental import pallas as pl
from jax.experimental.pallas import tpu as pltpu
from jax.sharding import PartitionSpec as P

PRE_SCALE = 144
MASKED = -1e30
MESH = pl.DeviceIdType.MESH
CHUNKS = 3
LAG = 4


def kernel(
    n, window, x_hbm, wq_hbm, wk_hbm, wv_hbm, wo_hbm, lens_ref, freq_ref, out_ref,
    tok, wq, w_kv, wo, cosv, sinv, query, mine, theirs, kv, att, first, acc,
    load_sem, ag_send, ag_recv, pair_send, pair_recv, sp_send, sp_recv, rs_send, rs_recv,
):
    z = lax.axis_index("tp")
    s = lax.axis_index("sp")
    right, left = lax.rem(z + 1, n), lax.rem(z + n - 1, n)
    parity = lax.rem(z, 2)
    pair = z + 1 - 2 * parity
    other = 1 - s
    side = (right, left)
    half = n // 2
    lag = min(LAG, half - 1)
    rows, depth = x_hbm.shape
    hd = wq_hbm.shape[1]
    hh = hd // 2
    sub = rows // CHUNKS
    width = depth // CHUNKS

    def block(offset):
        return lax.rem(z + offset + 2 * n, n)

    def load(src, dst, i):
        return pltpu.make_async_copy(src, dst, load_sem.at[i])

    own_load = load(x_hbm, tok.at[z], 0)
    loads = (
        load(wq_hbm, wq, 1),
        load(wk_hbm, w_kv.at[pl.ds(0, hh), :], 2),
        load(wv_hbm, w_kv.at[pl.ds(hh, hh), :], 3),
        load(wo_hbm, wo, 4),
    )

    def gather_copy(d, hop, b, c):
        piece = tok.at[b, pl.ds(c * sub, sub), :]
        return pltpu.make_async_remote_copy(
            src_ref=piece, dst_ref=piece,
            send_sem=ag_send.at[d, hop, c], recv_sem=ag_recv.at[d, hop, c],
            device_id={"tp": side[d]}, device_id_type=MESH,
        )

    def pair_copy(b):
        return pltpu.make_async_remote_copy(
            src_ref=mine.at[b], dst_ref=theirs.at[b],
            send_sem=pair_send.at[b], recv_sem=pair_recv.at[b],
            device_id={"tp": pair}, device_id_type=MESH,
        )

    def core_copy(b, core):
        piece = kv.at[pl.ds(pl.multiple_of((2 * b + core) * rows, 16), rows), :]
        return pltpu.make_async_remote_copy(
            src_ref=piece, dst_ref=piece,
            send_sem=sp_send.at[b], recv_sem=sp_recv.at[b],
            device_id={"sp": other}, device_id_type=MESH,
        )

    def sum_copy(d, hop, src, c):
        return pltpu.make_async_remote_copy(
            src_ref=src, dst_ref=acc.at[d, hop, c],
            send_sem=rs_send.at[d, hop, c], recv_sem=rs_recv.at[d, hop, c],
            device_id={"tp": side[d]}, device_id_type=MESH,
        )

    lane = lax.broadcasted_iota(jnp.int32, (rows, hd), 1)
    low = lane < hh
    even_mask = (lane * 0 + parity) == 0

    def turn(v, b):
        return v * cosv[b] + pltpu.roll(v, hh, 1) * sinv[b]

    def project(b):
        made = jnp.dot(tok[b], wq[...], preferred_element_type=jnp.float32)
        shared = lax.dot_general(
            tok[b], w_kv[...], (((1,), (1,)), ((), ())), preferred_element_type=jnp.float32
        )
        places = (2 * b + s) * rows + lax.broadcasted_iota(jnp.int32, (rows, hd), 0)
        angles = places.astype(jnp.float32) * freq_ref[...]
        cosv[b] = jnp.cos(angles)
        sine = jnp.sin(angles)
        sinv[b] = jnp.where(low, -sine, sine)
        query[b] = (turn(made, b) * PRE_SCALE ** (-0.5)).astype(jnp.bfloat16)
        mine[b] = shared.astype(jnp.bfloat16)

    def assemble(b):
        pair_copy(b).wait_recv()
        here = mine[b].astype(jnp.float32)
        there = theirs[b].astype(jnp.float32)
        lower = jnp.where(even_mask, here, there)
        upper = jnp.where(even_mask, there, here)
        key_raw = jnp.where(low, lower, pltpu.roll(upper, hh, 1))
        value = jnp.where(low, pltpu.roll(lower, hh, 1), upper)
        at = pl.ds(pl.multiple_of((2 * b + s) * rows, 16), rows)
        kv[at, pl.ds(0, hd)] = turn(key_raw, b).astype(jnp.bfloat16)
        kv[at, pl.ds(hd, hd)] = value.astype(jnp.bfloat16)
        core_copy(b, s).start()

    def attend(b, slot):
        start = pl.multiple_of(jnp.maximum((2 * b + s + 1) * rows - window, 0), 16)
        keys = kv[pl.ds(start, window), pl.ds(0, hd)]
        values = kv[pl.ds(start, window), pl.ds(hd, hd)]
        scores = lax.dot_general(
            query[b], keys, (((1,), (1,)), ((), ())), preferred_element_type=jnp.float32
        )
        place = (2 * b + s) * rows + lax.broadcasted_iota(jnp.int32, (rows, 1), 0)
        opens = jnp.zeros((rows, 1), jnp.int32)
        end = jnp.int32(0)
        for j in range(lens_ref.shape[0]):
            end = end + lens_ref[j]
            opens = jnp.where(place >= end, end, opens)
        key_place = start + lax.broadcasted_iota(jnp.int32, (rows, window), 1)
        allowed = (key_place <= place) & (key_place >= opens)
        masked = jnp.where(allowed, scores, MASKED)
        largest = jnp.max(masked, axis=1, keepdims=True)
        weights = jnp.where(allowed, jnp.exp(masked - largest), 0.0)
        denominator = jnp.sum(weights, axis=1, keepdims=True)
        mixed = jnp.dot(
            weights.astype(jnp.bfloat16), values, preferred_element_type=jnp.float32
        )
        att[slot] = (mixed / denominator).astype(jnp.bfloat16)

    def partial(slot, c):
        return jnp.dot(
            att[slot], wo[:, pl.ds(c * width, width)], preferred_element_type=jnp.float32
        )

    own_load.start()
    for copy in loads:
        copy.start()
    barrier = pltpu.get_barrier_semaphore()
    for where in ({"tp": left}, {"tp": right}, {"sp": other}):
        pl.semaphore_signal(barrier, inc=1, device_id=where, device_id_type=MESH)
    pl.semaphore_wait(barrier, 3)
    own_load.wait()
    for c in range(CHUNKS):
        for d in range(2):
            gather_copy(d, 0, z, c).start()
    for copy in loads:
        copy.wait()
    project(z)
    pair_copy(z).start()

    def gather_step(t, _):
        came = (block(-1 - t), block(1 + t))
        for c in range(CHUNKS):
            for d in range(2):
                gather_copy(d, t, came[d], c).wait_recv()

                @pl.when((t < half - 2) | (parity == 1 - d))
                def _():
                    gather_copy(d, t + 1, came[d], c).start()

            if c == 0:

                @pl.when(t == lag - 1)
                def _():
                    assemble(z)

                @pl.when(t >= lag)
                def _():
                    assemble(block(lag - 1 - t))
                    assemble(block(t + 1 - lag))

        for b in came:
            project(b)
            pair_copy(b).start()
        return 0

    lax.fori_loop(0, half - 1, gather_step, 0)
    far = block(half)
    for u in range(half - 1 - lag, half - 2):
        assemble(block(-1 - u))
        assemble(block(1 + u))
    for c in range(CHUNKS):
        for d in range(2):

            @pl.when(parity == d)
            def _():
                gather_copy(d, half - 1, far, c).wait_recv()

    project(far)
    pair_copy(far).start()
    for b in (far, block(half - 1), block(1 - half)):
        assemble(b)

    def core_arrival(b, _):
        core_copy(b, other).wait_recv()
        return 0

    lax.fori_loop(0, n, core_arrival, 0)

    attend(far, 0)
    for c in range(CHUNKS):
        first[c] = partial(0, c).astype(jnp.bfloat16)
        for d in range(2):

            @pl.when(s == d)
            def _():
                sum_copy(d, 0, first.at[c], c).start()

    attend(block(half - 1), 0)
    attend(block(1 - half), 1)

    def sum_step(t, _):
        for c in range(CHUNKS):
            for d in range(2):
                term = partial(d, c)
                here = acc.at[d, t - 1, c]
                arrives = (t > 1) | (s == d)

                @pl.when(arrives)
                def _():
                    sum_copy(d, t - 1, here, c).wait_recv()
                    here[...] = (here[...].astype(jnp.float32) + term).astype(jnp.bfloat16)

                @pl.when(jnp.logical_not(arrives))
                def _():
                    here[...] = term.astype(jnp.bfloat16)

                sum_copy(d, t, here, c).start()
        attend(block(half - 1 - t), 0)
        attend(block(t + 1 - half), 1)
        for b in (2 * t, 2 * t + 1):
            pair_copy(b).wait_send()
            core_copy(b, s).wait_send()
        for c in range(CHUNKS):
            for d in range(2):
                gather_copy(d, t - 1, z, c).wait_send()

                @pl.when((t > 2) | ((t == 2) & (s == d)))
                def _():
                    sum_copy(d, t - 2, first.at[c], c).wait_send()

        return 0

    lax.fori_loop(1, half, sum_step, 0)
    for c in range(CHUNKS):
        term = partial(0, c)
        for d in range(2):
            sum_copy(d, half - 1, acc.at[d, half - 1, c], c).wait_recv()
            term = term + acc[d, half - 1, c].astype(jnp.float32)
        out_ref[:, pl.ds(c * width, width)] = term.astype(jnp.bfloat16)

    for b in range(2):
        pair_copy(b).wait_send()
        core_copy(b, s).wait_send()
    for c in range(CHUNKS):
        for d in range(2):

            @pl.when(parity == 1 - d)
            def _():
                gather_copy(d, half - 1, z, c).wait_send()

            for hop in (half - 2, half - 1):
                sum_copy(d, hop, first.at[c], c).wait_send()


def layer(n, cores, tokens, w_query, w_key, w_value, w_out, doc_lengths):
    rows, depth = tokens.shape
    hd = w_query.shape[1]
    half = n // 2
    total = n * cores * rows
    longest = total // 4
    window = min(-(-(longest + rows) // 128) * 128, total)
    width = depth // CHUNKS
    spread = np.power(
        np.float32(10000.0), -(np.arange(hd // 2, dtype=np.float32) * np.float32(2.0 / hd))
    ).astype(np.float32)
    freq = jnp.asarray(np.concatenate([spread, spread])[None, :])
    anywhere = pl.BlockSpec(memory_space=pl.ANY)
    vmem = pl.BlockSpec(memory_space=pltpu.VMEM)
    bf16, f32, dma = jnp.bfloat16, jnp.float32, pltpu.SemaphoreType.DMA
    return pl.pallas_call(
        functools.partial(kernel, n, window),
        out_shape=jax.ShapeDtypeStruct((rows, depth), bf16),
        in_specs=[anywhere] * 5 + [pl.BlockSpec(memory_space=pltpu.SMEM), vmem],
        out_specs=vmem,
        scratch_shapes=[
            pltpu.VMEM((n, rows, depth), bf16),
            pltpu.VMEM((depth, hd), bf16),
            pltpu.VMEM((hd, depth), bf16),
            pltpu.VMEM((hd, depth), bf16),
            pltpu.VMEM((n, rows, hd), f32),
            pltpu.VMEM((n, rows, hd), f32),
            pltpu.VMEM((n, rows, hd), bf16),
            pltpu.VMEM((n, rows, hd), bf16),
            pltpu.VMEM((n, rows, hd), bf16),
            pltpu.VMEM((total, 2 * hd), bf16),
            pltpu.VMEM((2, rows, hd), bf16),
            pltpu.VMEM((CHUNKS, rows, width), bf16),
            pltpu.VMEM((2, half, CHUNKS, rows, width), bf16),
            dma((5,)),
            dma((2, half, CHUNKS)),
            dma((2, half, CHUNKS)),
            dma((n,)),
            dma((n,)),
            dma((n,)),
            dma((n,)),
            dma((2, half, CHUNKS)),
            dma((2, half, CHUNKS)),
        ],
        compiler_params=pltpu.CompilerParams(
            collective_id=0, has_side_effects=True, vmem_limit_bytes=60 * 1024 * 1024
        ),
    )(tokens, w_query, w_key.T, w_value.T, w_out, doc_lengths, freq)


def solution(mesh):
    placed = (
        P(("groups", "tp", "sp"), None),
        P(None, "tp"),
        P(None, "tp"),
        P(None, "tp"),
        P("tp", None),
        P("groups"),
    )
    return jax.shard_map(
        functools.partial(layer, mesh.shape["tp"], mesh.shape["sp"]),
        mesh=mesh,
        in_specs=placed,
        out_specs=P(("groups", "tp", "sp"), None),
        check_vma=False,
    )
```

```python
import functools
import math

import jax
import jax.numpy as jnp
import numpy as np
from jax import lax
from jax.experimental import pallas as pl
from jax.experimental.pallas import tpu as pltpu
from jax.sharding import PartitionSpec as P

PRE_SCALE = 144
MASKED = -1e30
MESH = pl.DeviceIdType.MESH
CHUNKS = 3
LAG = 4


def kernel(
    n, window, x_hbm, wq_hbm, wk_hbm, wv_hbm, wo_hbm, lens_ref, freq_ref, out_ref,
    tok, wq, w_kv, wo, cosv, sinv, query, mine, theirs, kv, att, first, acc,
    load_sem, ag_send, ag_recv, pair_send, pair_recv, sp_send, sp_recv, rs_send, rs_recv,
):
    z = lax.axis_index("tp")
    s = lax.axis_index("sp")
    right, left = lax.rem(z + 1, n), lax.rem(z + n - 1, n)
    parity = lax.rem(z, 2)
    pair = z + 1 - 2 * parity
    other = 1 - s
    side = (right, left)
    half = n // 2
    lag = min(LAG, half - 1)
    rows, depth = x_hbm.shape
    hd = wq_hbm.shape[1]
    hh = hd // 2
    sub = rows // CHUNKS
    width = depth // CHUNKS

    def block(offset):
        return lax.rem(z + offset + 2 * n, n)

    def load(src, dst, i):
        return pltpu.make_async_copy(src, dst, load_sem.at[i])

    own_load = load(x_hbm, tok.at[z], 0)
    loads = (
        load(wq_hbm, wq, 1),
        load(wk_hbm, w_kv.at[pl.ds(0, hh), :], 2),
        load(wv_hbm, w_kv.at[pl.ds(hh, hh), :], 3),
        load(wo_hbm, wo, 4),
    )

    def gather_copy(d, hop, b, c):
        piece = tok.at[b, pl.ds(c * sub, sub), :]
        return pltpu.make_async_remote_copy(
            src_ref=piece, dst_ref=piece,
            send_sem=ag_send.at[0], recv_sem=ag_recv.at[d, hop, c],
            device_id={"tp": side[d]}, device_id_type=MESH,
        )

    def pair_copy(b):
        return pltpu.make_async_remote_copy(
            src_ref=mine.at[b], dst_ref=theirs.at[b],
            send_sem=pair_send.at[0], recv_sem=pair_recv.at[b],
            device_id={"tp": pair}, device_id_type=MESH,
        )

    def core_copy(b, core):
        piece = kv.at[pl.ds(pl.multiple_of((2 * b + core) * rows, 16), rows), :]
        return pltpu.make_async_remote_copy(
            src_ref=piece, dst_ref=piece,
            send_sem=sp_send.at[0], recv_sem=sp_recv.at[0],
            device_id={"sp": other}, device_id_type=MESH,
        )

    def sum_copy(d, hop, src, c, stage=1):
        return pltpu.make_async_remote_copy(
            src_ref=src, dst_ref=acc.at[d, hop, c],
            send_sem=rs_send.at[stage], recv_sem=rs_recv.at[d, hop, c],
            device_id={"tp": side[d]}, device_id_type=MESH,
        )

    def whole(ref, send, recv, where):
        return pltpu.make_async_remote_copy(
            src_ref=ref, dst_ref=ref, send_sem=send, recv_sem=recv,
            device_id=where, device_id_type=MESH,
        )

    lane = lax.broadcasted_iota(jnp.int32, (rows, hd), 1)
    low = lane < hh
    even_mask = (lane * 0 + parity) == 0

    def turn(v, b):
        return v * cosv[b] + pltpu.roll(v, hh, 1) * sinv[b]

    def project(b):
        shared = lax.dot_general(
            tok[b], w_kv[...], (((1,), (1,)), ((), ())), preferred_element_type=jnp.float32
        )
        mine[b] = shared.astype(jnp.bfloat16)
        pair_copy(b).start()
        made = jnp.dot(tok[b], wq[...], preferred_element_type=jnp.float32)
        places = (2 * b + s) * rows + lax.broadcasted_iota(jnp.int32, (rows, hd), 0)
        angles = places.astype(jnp.float32) * freq_ref[...]
        cosv[b] = jnp.cos(angles)
        sine = jnp.sin(angles)
        sinv[b] = jnp.where(low, -sine, sine)
        query[b] = (turn(made, b) * PRE_SCALE ** (-0.5)).astype(jnp.bfloat16)

    def assemble(b):
        pair_copy(b).wait_recv()
        here = mine[b].astype(jnp.float32)
        there = theirs[b].astype(jnp.float32)
        lower = jnp.where(even_mask, here, there)
        upper = jnp.where(even_mask, there, here)
        key_raw = jnp.where(low, lower, pltpu.roll(upper, hh, 1))
        value = jnp.where(low, pltpu.roll(lower, hh, 1), upper)
        at = pl.ds(pl.multiple_of((2 * b + s) * rows, 16), rows)
        kv[at, pl.ds(0, hd)] = turn(key_raw, b).astype(jnp.bfloat16)
        kv[at, pl.ds(hd, hd)] = value.astype(jnp.bfloat16)
        core_copy(b, s).start()

    def attend(b, slot):
        start = pl.multiple_of(jnp.maximum((2 * b + s + 1) * rows - window, 0), 16)
        keys = kv[pl.ds(start, window), pl.ds(0, hd)]
        values = kv[pl.ds(start, window), pl.ds(hd, hd)]
        scores = lax.dot_general(
            query[b], keys, (((1,), (1,)), ((), ())), preferred_element_type=jnp.float32
        )
        place = (2 * b + s) * rows + lax.broadcasted_iota(jnp.int32, (rows, 1), 0)
        opens = jnp.zeros((rows, 1), jnp.int32)
        end = jnp.int32(0)
        for j in range(lens_ref.shape[0]):
            end = end + lens_ref[j]
            opens = jnp.where(place >= end, end, opens)
        key_place = start + lax.broadcasted_iota(jnp.int32, (rows, window), 1)
        allowed = (key_place <= place) & (key_place >= opens)
        masked = jnp.where(allowed, scores, MASKED)
        largest = jnp.max(masked, axis=1, keepdims=True)
        weights = jnp.where(allowed, jnp.exp(masked - largest), 0.0)
        denominator = jnp.sum(weights, axis=1, keepdims=True)
        mixed = jnp.dot(
            weights.astype(jnp.bfloat16), values, preferred_element_type=jnp.float32
        )
        att[slot] = (mixed / denominator).astype(jnp.bfloat16)

    def partial(slot, c):
        return jnp.dot(
            att[slot], wo[:, pl.ds(c * width, width)], preferred_element_type=jnp.float32
        )

    own_load.start()
    for copy in loads:
        copy.start()
    barrier = pltpu.get_barrier_semaphore()
    for where in ({"tp": left}, {"tp": right}, {"sp": other}):
        pl.semaphore_signal(barrier, inc=1, device_id=where, device_id_type=MESH)
    pl.semaphore_wait(barrier, 3)
    own_load.wait()
    for c in range(CHUNKS):
        for d in range(2):
            gather_copy(d, 0, z, c).start()
    for copy in loads:
        copy.wait()
    project(z)

    def gather_step(t, _):
        came = (block(-1 - t), block(1 + t))
        for c in range(CHUNKS):
            for d in range(2):
                gather_copy(d, t, came[d], c).wait_recv()

                @pl.when((t < half - 2) | (parity == 1 - d))
                def _():
                    gather_copy(d, t + 1, came[d], c).start()

            if c == 0:

                @pl.when(t == lag - 1)
                def _():
                    assemble(z)

                @pl.when(t >= lag)
                def _():
                    assemble(block(lag - 1 - t))
                    assemble(block(t + 1 - lag))

        for b in came:
            project(b)
        return 0

    lax.fori_loop(0, half - 1, gather_step, 0)
    far = block(half)
    for u in range(half - 1 - lag, half - 2):
        assemble(block(-1 - u))
        assemble(block(1 + u))
    assemble(block((1 - 2 * parity) * (half - 1)))
    for c in range(CHUNKS):
        for d in range(2):

            @pl.when(parity == d)
            def _():
                gather_copy(d, half - 1, far, c).wait_recv()

    project(far)
    assemble(far)
    assemble(block((2 * parity - 1) * (half - 1)))
    cores_kv = whole(kv.at[pl.ds(0, n * rows), :], sp_send.at[0], sp_recv.at[0], {"sp": other})
    cores_kv.wait_recv()

    attend(far, 0)
    for c in range(CHUNKS):
        first[c] = partial(0, c).astype(jnp.bfloat16)
        for d in range(2):

            @pl.when(s == d)
            def _():
                sum_copy(d, 0, first.at[c], c, 0).start()

    attend(block(half - 1), 0)
    attend(block(1 - half), 1)

    def sum_step(t, _):
        for c in range(CHUNKS):
            for d in range(2):
                term = partial(d, c)
                here = acc.at[d, t - 1, c]
                arrives = (t > 1) | (s == d)

                @pl.when(arrives)
                def _():
                    sum_copy(d, t - 1, here, c).wait_recv()
                    here[...] = (here[...].astype(jnp.float32) + term).astype(jnp.bfloat16)

                @pl.when(jnp.logical_not(arrives))
                def _():
                    here[...] = term.astype(jnp.bfloat16)

                sum_copy(d, t, here, c).start()
        attend(block(half - 1 - t), 0)
        attend(block(t + 1 - half), 1)
        return 0

    lax.fori_loop(1, half, sum_step, 0)
    for c in range(CHUNKS):
        term = partial(0, c)
        for d in range(2):
            sum_copy(d, half - 1, acc.at[d, half - 1, c], c).wait_recv()
            term = term + acc[d, half - 1, c].astype(jnp.float32)
        out_ref[:, pl.ds(c * width, width)] = term.astype(jnp.bfloat16)

    cores_kv.wait_send()
    ring = {"tp": right}
    whole(mine, pair_send.at[0], pair_recv.at[0], ring).wait_send()
    whole(tok.at[pl.ds(0, n - 1)], ag_send.at[0], ag_recv.at[0, 0, 0], ring).wait_send()
    whole(first, rs_send.at[0], rs_recv.at[0, 0, 0], ring).wait_send()
    whole(acc.at[:, pl.ds(0, half - 1)], rs_send.at[1], rs_recv.at[0, 0, 0], ring).wait_send()


def layer(n, cores, tokens, w_query, w_key, w_value, w_out, doc_lengths):
    rows, depth = tokens.shape
    hd = w_query.shape[1]
    half = n // 2
    total = n * cores * rows
    longest = total // 4
    window = min(-(-(longest + rows) // 128) * 128, total)
    width = depth // CHUNKS
    spread = np.power(
        np.float32(10000.0), -(np.arange(hd // 2, dtype=np.float32) * np.float32(2.0 / hd))
    ).astype(np.float32)
    freq = jnp.asarray(np.concatenate([spread, spread])[None, :])
    anywhere = pl.BlockSpec(memory_space=pl.ANY)
    vmem = pl.BlockSpec(memory_space=pltpu.VMEM)
    bf16, f32, dma = jnp.bfloat16, jnp.float32, pltpu.SemaphoreType.DMA
    return pl.pallas_call(
        functools.partial(kernel, n, window),
        out_shape=jax.ShapeDtypeStruct((rows, depth), bf16),
        in_specs=[anywhere] * 5 + [pl.BlockSpec(memory_space=pltpu.SMEM), vmem],
        out_specs=vmem,
        scratch_shapes=[
            pltpu.VMEM((n, rows, depth), bf16),
            pltpu.VMEM((depth, hd), bf16),
            pltpu.VMEM((hd, depth), bf16),
            pltpu.VMEM((hd, depth), bf16),
            pltpu.VMEM((n, rows, hd), f32),
            pltpu.VMEM((n, rows, hd), f32),
            pltpu.VMEM((n, rows, hd), bf16),
            pltpu.VMEM((n, rows, hd), bf16),
            pltpu.VMEM((n, rows, hd), bf16),
            pltpu.VMEM((total, 2 * hd), bf16),
            pltpu.VMEM((2, rows, hd), bf16),
            pltpu.VMEM((CHUNKS, rows, width), bf16),
            pltpu.VMEM((2, half, CHUNKS, rows, width), bf16),
            dma((5,)),
            dma((1,)),
            dma((2, half, CHUNKS)),
            dma((1,)),
            dma((n,)),
            dma((1,)),
            dma((1,)),
            dma((2,)),
            dma((2, half, CHUNKS)),
        ],
        compiler_params=pltpu.CompilerParams(
            collective_id=0, has_side_effects=True, vmem_limit_bytes=60 * 1024 * 1024
        ),
    )(tokens, w_query, w_key.T, w_value.T, w_out, doc_lengths, freq)


def solution(mesh):
    placed = (
        P(("groups", "tp", "sp"), None),
        P(None, "tp"),
        P(None, "tp"),
        P(None, "tp"),
        P("tp", None),
        P("groups"),
    )
    return jax.shard_map(
        functools.partial(layer, mesh.shape["tp"], mesh.shape["sp"]),
        mesh=mesh,
        in_specs=placed,
        out_specs=P(("groups", "tp", "sp"), None),
        check_vma=False,
    )
```

```python
import functools
import math

import jax
import jax.numpy as jnp
import numpy as np
from jax import lax
from jax.experimental import pallas as pl
from jax.experimental.pallas import tpu as pltpu
from jax.sharding import PartitionSpec as P

PRE_SCALE = 144
MASKED = -1e30
MESH = pl.DeviceIdType.MESH
CHUNKS = 3
SLOTS = 4


def kernel(
    n, window, x_hbm, wq_hbm, wk_hbm, wv_hbm, wo_hbm, lens_ref, freq_ref, out_ref,
    tok, wq, w_kv, wo, cosv, sinv, query, mine, theirs, kv, att, first, acc,
    load_sem, ag_send, ag_recv, pair_send, pair_recv, sp_send, sp_recv, rs_send, rs_recv,
):
    z = lax.axis_index("tp")
    s = lax.axis_index("sp")
    right, left = lax.rem(z + 1, n), lax.rem(z + n - 1, n)
    parity = lax.rem(z, 2)
    pair = z + 1 - 2 * parity
    other = 1 - s
    side = (right, left)
    half = n // 2
    rows, depth = x_hbm.shape
    hd = wq_hbm.shape[1]
    hh = hd // 2
    sub = rows // CHUNKS
    width = depth // CHUNKS

    def block(offset):
        return lax.rem(z + offset + 2 * n, n)

    def load(src, dst, i):
        return pltpu.make_async_copy(src, dst, load_sem.at[i])

    own_load = load(x_hbm, tok.at[z], 0)
    loads = (
        load(wq_hbm, wq, 1),
        load(wk_hbm, w_kv.at[pl.ds(0, hh), :], 2),
        load(wv_hbm, w_kv.at[pl.ds(hh, hh), :], 3),
        load(wo_hbm, wo, 4),
    )

    def gather_copy(d, hop, b, c):
        piece = tok.at[b, pl.ds(c * sub, sub), :]
        return pltpu.make_async_remote_copy(
            src_ref=piece, dst_ref=piece,
            send_sem=ag_send.at[0], recv_sem=ag_recv.at[d, lax.rem(hop, SLOTS), c],
            device_id={"tp": side[d]}, device_id_type=MESH,
        )

    def pair_copy(b):
        return pltpu.make_async_remote_copy(
            src_ref=mine.at[b], dst_ref=theirs.at[b],
            send_sem=pair_send.at[0], recv_sem=pair_recv.at[b],
            device_id={"tp": pair}, device_id_type=MESH,
        )

    def core_copy(b, core):
        piece = kv.at[pl.ds(pl.multiple_of((2 * b + core) * rows, 16), rows), :]
        return pltpu.make_async_remote_copy(
            src_ref=piece, dst_ref=piece,
            send_sem=sp_send.at[0], recv_sem=sp_recv.at[0],
            device_id={"sp": other}, device_id_type=MESH,
        )

    def sum_copy(d, hop, src, c, stage=1):
        return pltpu.make_async_remote_copy(
            src_ref=src, dst_ref=acc.at[d, hop, c],
            send_sem=rs_send.at[stage], recv_sem=rs_recv.at[d, lax.rem(hop, SLOTS), c],
            device_id={"tp": side[d]}, device_id_type=MESH,
        )

    def whole(ref, send, recv, where):
        return pltpu.make_async_remote_copy(
            src_ref=ref, dst_ref=ref, send_sem=send, recv_sem=recv,
            device_id=where, device_id_type=MESH,
        )

    lane = lax.broadcasted_iota(jnp.int32, (rows, hd), 1)
    low = lane < hh
    even_mask = (lane * 0 + parity) == 0

    def turn(v, b):
        return v * cosv[b] + pltpu.roll(v, hh, 1) * sinv[b]

    def project(b, send=False):
        shared = lax.dot_general(
            tok[b], w_kv[...], (((1,), (1,)), ((), ())), preferred_element_type=jnp.float32
        )
        mine[b] = shared.astype(jnp.bfloat16)
        if send:
            pair_copy(b).start()
        made = jnp.dot(tok[b], wq[...], preferred_element_type=jnp.float32)
        places = (2 * b + s) * rows + lax.broadcasted_iota(jnp.int32, (rows, hd), 0)
        angles = places.astype(jnp.float32) * freq_ref[...]
        cosv[b] = jnp.cos(angles)
        sine = jnp.sin(angles)
        sinv[b] = jnp.where(low, -sine, sine)
        query[b] = (turn(made, b) * PRE_SCALE ** (-0.5)).astype(jnp.bfloat16)

    def assemble(b):
        pair_copy(b).wait_recv()
        here = mine[b].astype(jnp.float32)
        there = theirs[b].astype(jnp.float32)
        lower = jnp.where(even_mask, here, there)
        upper = jnp.where(even_mask, there, here)
        key_raw = jnp.where(low, lower, pltpu.roll(upper, hh, 1))
        value = jnp.where(low, pltpu.roll(lower, hh, 1), upper)
        at = pl.ds(pl.multiple_of((2 * b + s) * rows, 16), rows)
        kv[at, pl.ds(0, hd)] = turn(key_raw, b).astype(jnp.bfloat16)
        kv[at, pl.ds(hd, hd)] = value.astype(jnp.bfloat16)
        core_copy(b, s).start()

    def attend(b, slot):
        start = pl.multiple_of(jnp.maximum((2 * b + s + 1) * rows - window, 0), 16)
        keys = kv[pl.ds(start, window), pl.ds(0, hd)]
        values = kv[pl.ds(start, window), pl.ds(hd, hd)]
        scores = lax.dot_general(
            query[b], keys, (((1,), (1,)), ((), ())), preferred_element_type=jnp.float32
        )
        place = (2 * b + s) * rows + lax.broadcasted_iota(jnp.int32, (rows, 1), 0)
        opens = jnp.zeros((rows, 1), jnp.int32)
        end = jnp.int32(0)
        for j in range(lens_ref.shape[0]):
            end = end + lens_ref[j]
            opens = jnp.where(place >= end, end, opens)
        key_place = start + lax.broadcasted_iota(jnp.int32, (rows, window), 1)
        allowed = (key_place <= place) & (key_place >= opens)
        masked = jnp.where(allowed, scores, MASKED)
        largest = jnp.max(masked, axis=1, keepdims=True)
        weights = jnp.where(allowed, jnp.exp(masked - largest), 0.0)
        denominator = jnp.sum(weights, axis=1, keepdims=True)
        mixed = jnp.dot(
            weights.astype(jnp.bfloat16), values, preferred_element_type=jnp.float32
        )
        att[slot] = (mixed / denominator).astype(jnp.bfloat16)

    def partial(slot, c):
        return jnp.dot(
            att[slot], wo[:, pl.ds(c * width, width)], preferred_element_type=jnp.float32
        )

    own_load.start()
    for copy in loads:
        copy.start()
    barrier = pltpu.get_barrier_semaphore()
    for where in ({"tp": left}, {"tp": right}, {"sp": other}):
        pl.semaphore_signal(barrier, inc=1, device_id=where, device_id_type=MESH)
    pl.semaphore_wait(barrier, 3)
    own_load.wait()
    for c in range(CHUNKS):
        for d in range(2):
            gather_copy(d, 0, z, c).start()
    for copy in loads:
        copy.wait()
    project(z)

    def gather_step(t, _):
        came = (block(-1 - t), block(1 + t))
        for c in range(CHUNKS):
            for d in range(2):
                gather_copy(d, t, came[d], c).wait_recv()

                @pl.when((t < half - 2) | (parity == 1 - d))
                def _():
                    gather_copy(d, t + 1, came[d], c).start()

        for b in came:
            project(b)

        @pl.when(t == half - 3)
        def _():
            def send_half(k, _):
                pair_copy(block(k + 2 - half)).start()
                return 0

            lax.fori_loop(0, 2 * half - 3, send_half, 0)

        @pl.when(t == half - 2)
        def _():
            for b in came:
                pair_copy(b).start()

        return 0

    lax.fori_loop(0, half - 1, gather_step, 0)
    far = block(half)

    def assemble_shared(k, _):
        assemble(block(k + 3 - half - parity))
        return 0

    lax.fori_loop(0, 2 * half - 4, assemble_shared, 0)
    assemble(block((2 * parity - 1) * (half - 2)))
    assemble(block((1 - 2 * parity) * (half - 1)))
    for c in range(CHUNKS):
        for d in range(2):

            @pl.when(parity == d)
            def _():
                gather_copy(d, half - 1, far, c).wait_recv()

    project(far, True)
    assemble(far)
    assemble(block((2 * parity - 1) * (half - 1)))
    cores_kv = whole(kv.at[pl.ds(0, n * rows), :], sp_send.at[0], sp_recv.at[0], {"sp": other})
    cores_kv.wait_recv()

    attend(far, 0)
    for c in range(CHUNKS):
        first[c] = partial(0, c).astype(jnp.bfloat16)
        for d in range(2):

            @pl.when(s == d)
            def _():
                sum_copy(d, 0, first.at[c], c, 0).start()

    attend(block(half - 1), 0)
    attend(block(1 - half), 1)

    def sum_step(t, _):
        for c in range(CHUNKS):
            for d in range(2):
                term = partial(d, c)
                here = acc.at[d, t - 1, c]
                arrives = (t > 1) | (s == d)

                @pl.when(arrives)
                def _():
                    sum_copy(d, t - 1, here, c).wait_recv()
                    here[...] = (here[...].astype(jnp.float32) + term).astype(jnp.bfloat16)

                @pl.when(jnp.logical_not(arrives))
                def _():
                    here[...] = term.astype(jnp.bfloat16)

                sum_copy(d, t, here, c).start()
        attend(block(half - 1 - t), 0)
        attend(block(t + 1 - half), 1)
        return 0

    lax.fori_loop(1, half, sum_step, 0)
    for c in range(CHUNKS):
        term = partial(0, c)
        for d in range(2):
            sum_copy(d, half - 1, acc.at[d, half - 1, c], c).wait_recv()
            term = term + acc[d, half - 1, c].astype(jnp.float32)
        out_ref[:, pl.ds(c * width, width)] = term.astype(jnp.bfloat16)

    cores_kv.wait_send()
    ring = {"tp": right}
    whole(mine, pair_send.at[0], pair_recv.at[0], ring).wait_send()
    whole(tok.at[pl.ds(0, n - 1)], ag_send.at[0], ag_recv.at[0, 0, 0], ring).wait_send()
    whole(first, rs_send.at[0], rs_recv.at[0, 0, 0], ring).wait_send()
    whole(acc.at[:, pl.ds(0, half - 1)], rs_send.at[1], rs_recv.at[0, 0, 0], ring).wait_send()


def layer(n, cores, tokens, w_query, w_key, w_value, w_out, doc_lengths):
    rows, depth = tokens.shape
    hd = w_query.shape[1]
    half = n // 2
    total = n * cores * rows
    longest = total // 4
    window = min(-(-(longest + rows) // 128) * 128, total)
    width = depth // CHUNKS
    spread = np.power(
        np.float32(10000.0), -(np.arange(hd // 2, dtype=np.float32) * np.float32(2.0 / hd))
    ).astype(np.float32)
    freq = jnp.asarray(np.concatenate([spread, spread])[None, :])
    anywhere = pl.BlockSpec(memory_space=pl.ANY)
    vmem = pl.BlockSpec(memory_space=pltpu.VMEM)
    bf16, f32, dma = jnp.bfloat16, jnp.float32, pltpu.SemaphoreType.DMA
    return pl.pallas_call(
        functools.partial(kernel, n, window),
        out_shape=jax.ShapeDtypeStruct((rows, depth), bf16),
        in_specs=[anywhere] * 5 + [pl.BlockSpec(memory_space=pltpu.SMEM), vmem],
        out_specs=vmem,
        scratch_shapes=[
            pltpu.VMEM((n, rows, depth), bf16),
            pltpu.VMEM((depth, hd), bf16),
            pltpu.VMEM((hd, depth), bf16),
            pltpu.VMEM((hd, depth), bf16),
            pltpu.VMEM((n, rows, hd), f32),
            pltpu.VMEM((n, rows, hd), f32),
            pltpu.VMEM((n, rows, hd), bf16),
            pltpu.VMEM((n, rows, hd), bf16),
            pltpu.VMEM((n, rows, hd), bf16),
            pltpu.VMEM((total, 2 * hd), bf16),
            pltpu.VMEM((2, rows, hd), bf16),
            pltpu.VMEM((CHUNKS, rows, width), bf16),
            pltpu.VMEM((2, half, CHUNKS, rows, width), bf16),
            dma((5,)),
            dma((1,)),
            dma((2, SLOTS, CHUNKS)),
            dma((1,)),
            dma((n,)),
            dma((1,)),
            dma((1,)),
            dma((2,)),
            dma((2, SLOTS, CHUNKS)),
        ],
        compiler_params=pltpu.CompilerParams(
            collective_id=0, has_side_effects=True, vmem_limit_bytes=60 * 1024 * 1024
        ),
    )(tokens, w_query, w_key.T, w_value.T, w_out, doc_lengths, freq)


def solution(mesh):
    placed = (
        P(("groups", "tp", "sp"), None),
        P(None, "tp"),
        P(None, "tp"),
        P(None, "tp"),
        P("tp", None),
        P("groups"),
    )
    return jax.shard_map(
        functools.partial(layer, mesh.shape["tp"], mesh.shape["sp"]),
        mesh=mesh,
        in_specs=placed,
        out_specs=P(("groups", "tp", "sp"), None),
        check_vma=False,
    )
```

```python
import functools
import math

import jax
import jax.numpy as jnp
import numpy as np
from jax import lax
from jax.experimental import pallas as pl
from jax.experimental.pallas import tpu as pltpu
from jax.sharding import PartitionSpec as P

PRE_SCALE = 144
MASKED = -1e30
MESH = pl.DeviceIdType.MESH
CHUNKS = 3
SLOTS = 3


def kernel(
    n, window, x_hbm, wq_hbm, wk_hbm, wv_hbm, wo_hbm, lens_ref, freq_ref, out_ref,
    tok, wq, w_kv, wo, cosv, sinv, query, mine, theirs, kv, att, first, acc,
    load_sem, ag_send, ag_recv, pair_send, pair_recv, sp_send, sp_recv, rs_send, rs_recv,
):
    z = lax.axis_index("tp")
    s = lax.axis_index("sp")
    right, left = lax.rem(z + 1, n), lax.rem(z + n - 1, n)
    parity = lax.rem(z, 2)
    pair = z + 1 - 2 * parity
    other = 1 - s
    side = (right, left)
    half = n // 2
    rows, depth = x_hbm.shape
    hd = wq_hbm.shape[1]
    hh = hd // 2
    sub = rows // CHUNKS
    width = depth // CHUNKS

    def block(offset):
        return lax.rem(z + offset + 2 * n, n)

    def load(src, dst, i):
        return pltpu.make_async_copy(src, dst, load_sem.at[i])

    own_load = load(x_hbm, tok.at[z], 0)
    loads = (
        load(wq_hbm, wq, 1),
        load(wk_hbm, w_kv.at[pl.ds(0, hh), :], 2),
        load(wv_hbm, w_kv.at[pl.ds(hh, hh), :], 3),
        load(wo_hbm, wo, 4),
    )

    def gather_copy(d, hop, b, c):
        piece = tok.at[b, pl.ds(c * sub, sub), :]
        return pltpu.make_async_remote_copy(
            src_ref=piece, dst_ref=piece,
            send_sem=ag_send.at[0], recv_sem=ag_recv.at[d, lax.rem(hop, SLOTS), c],
            device_id={"tp": side[d]}, device_id_type=MESH,
        )

    def pair_copy(b):
        return pltpu.make_async_remote_copy(
            src_ref=mine.at[b], dst_ref=theirs.at[b],
            send_sem=pair_send.at[0], recv_sem=pair_recv.at[b],
            device_id={"tp": pair}, device_id_type=MESH,
        )

    def core_copy(b, core):
        piece = kv.at[pl.ds(pl.multiple_of((2 * b + core) * rows, 16), rows), :]
        return pltpu.make_async_remote_copy(
            src_ref=piece, dst_ref=piece,
            send_sem=sp_send.at[0], recv_sem=sp_recv.at[0],
            device_id={"sp": other}, device_id_type=MESH,
        )

    def sum_copy(d, hop, src, c, stage=1):
        return pltpu.make_async_remote_copy(
            src_ref=src, dst_ref=acc.at[d, hop, c],
            send_sem=rs_send.at[stage], recv_sem=rs_recv.at[d, lax.rem(hop, SLOTS), c],
            device_id={"tp": side[d]}, device_id_type=MESH,
        )

    def whole(ref, send, recv, where):
        return pltpu.make_async_remote_copy(
            src_ref=ref, dst_ref=ref, send_sem=send, recv_sem=recv,
            device_id=where, device_id_type=MESH,
        )

    lane = lax.broadcasted_iota(jnp.int32, (rows, hd), 1)
    low = lane < hh
    even_mask = (lane * 0 + parity) == 0

    def turn(v, b):
        return v * cosv[b] + pltpu.roll(v, hh, 1) * sinv[b]

    def project(b, send=False):
        shared = lax.dot_general(
            tok[b], w_kv[...], (((1,), (1,)), ((), ())), preferred_element_type=jnp.float32
        )
        mine[b] = shared.astype(jnp.bfloat16)
        if send:
            pair_copy(b).start()
        made = jnp.dot(tok[b], wq[...], preferred_element_type=jnp.float32)
        places = (2 * b + s) * rows + lax.broadcasted_iota(jnp.int32, (rows, hd), 0)
        angles = places.astype(jnp.float32) * freq_ref[...]
        cosv[b] = jnp.cos(angles)
        sine = jnp.sin(angles)
        sinv[b] = jnp.where(low, -sine, sine)
        query[b] = (turn(made, b) * PRE_SCALE ** (-0.5)).astype(jnp.bfloat16)

    def assemble(b):
        pair_copy(b).wait_recv()
        here = mine[b].astype(jnp.float32)
        there = theirs[b].astype(jnp.float32)
        lower = jnp.where(even_mask, here, there)
        upper = jnp.where(even_mask, there, here)
        key_raw = jnp.where(low, lower, pltpu.roll(upper, hh, 1))
        value = jnp.where(low, pltpu.roll(lower, hh, 1), upper)
        at = pl.ds(pl.multiple_of((2 * b + s) * rows, 16), rows)
        kv[at, pl.ds(0, hd)] = turn(key_raw, b).astype(jnp.bfloat16)
        kv[at, pl.ds(hd, hd)] = value.astype(jnp.bfloat16)
        core_copy(b, s).start()

    def attend(b, slot):
        start = pl.multiple_of(jnp.maximum((2 * b + s + 1) * rows - window, 0), 16)
        keys = kv[pl.ds(start, window), pl.ds(0, hd)]
        values = kv[pl.ds(start, window), pl.ds(hd, hd)]
        scores = lax.dot_general(
            query[b], keys, (((1,), (1,)), ((), ())), preferred_element_type=jnp.float32
        )
        place = (2 * b + s) * rows + lax.broadcasted_iota(jnp.int32, (rows, 1), 0)
        opens = jnp.zeros((rows, 1), jnp.int32)
        end = jnp.int32(0)
        for j in range(lens_ref.shape[0]):
            end = end + lens_ref[j]
            opens = jnp.where(place >= end, end, opens)
        key_place = start + lax.broadcasted_iota(jnp.int32, (rows, window), 1)
        allowed = (key_place <= place) & (key_place >= opens)
        masked = jnp.where(allowed, scores, MASKED)
        largest = jnp.max(masked, axis=1, keepdims=True)
        weights = jnp.where(allowed, jnp.exp(masked - largest), 0.0)
        denominator = jnp.sum(weights, axis=1, keepdims=True)
        mixed = jnp.dot(
            weights.astype(jnp.bfloat16), values, preferred_element_type=jnp.float32
        )
        att[slot] = (mixed / denominator).astype(jnp.bfloat16)

    def partial(slot, c):
        return jnp.dot(
            att[slot], wo[:, pl.ds(c * width, width)], preferred_element_type=jnp.float32
        )

    own_load.start()
    for copy in loads:
        copy.start()
    barrier = pltpu.get_barrier_semaphore()
    for where in ({"tp": left}, {"tp": right}, {"sp": other}):
        pl.semaphore_signal(barrier, inc=1, device_id=where, device_id_type=MESH)
    pl.semaphore_wait(barrier, 3)
    own_load.wait()
    for c in range(CHUNKS):
        for d in range(2):
            gather_copy(d, 0, z, c).start()
    for copy in loads:
        copy.wait()
    project(z)

    def gather_step(t, _):
        came = (block(-1 - t), block(1 + t))
        for c in range(CHUNKS):
            for d in range(2):
                gather_copy(d, t, came[d], c).wait_recv()

                @pl.when((t < half - 2) | (parity == 1 - d))
                def _():
                    gather_copy(d, t + 1, came[d], c).start()

        for b in came:
            project(b)

        @pl.when(t == half - 3)
        def _():
            def send_half(k, _):
                pair_copy(block(k + 2 - half)).start()
                return 0

            lax.fori_loop(0, 2 * half - 3, send_half, 0)

        @pl.when(t == half - 2)
        def _():
            for b in came:
                pair_copy(b).start()

        return 0

    lax.fori_loop(0, half - 1, gather_step, 0)
    far = block(half)

    def assemble_shared(k, _):
        assemble(block(k + 3 - half - parity))
        return 0

    lax.fori_loop(0, 2 * half - 4, assemble_shared, 0)
    assemble(block((2 * parity - 1) * (half - 2)))
    assemble(block((1 - 2 * parity) * (half - 1)))
    for c in range(CHUNKS):
        for d in range(2):

            @pl.when(parity == d)
            def _():
                gather_copy(d, half - 1, far, c).wait_recv()

    project(far, True)
    assemble(far)
    assemble(block((2 * parity - 1) * (half - 1)))
    cores_kv = whole(kv.at[pl.ds(0, n * rows), :], sp_send.at[0], sp_recv.at[0], {"sp": other})
    cores_kv.wait_recv()

    attend(far, 0)
    for c in range(CHUNKS):
        first[c] = partial(0, c).astype(jnp.bfloat16)
        for d in range(2):

            @pl.when(s == d)
            def _():
                sum_copy(d, 0, first.at[c], c, 0).start()

    attend(block(half - 1), 0)
    attend(block(1 - half), 1)

    def sum_step(t, _):
        for c in range(CHUNKS):
            for d in range(2):
                term = partial(d, c)
                here = acc.at[d, t - 1, c]
                arrives = (t > 1) | (s == d)

                @pl.when(arrives)
                def _():
                    sum_copy(d, t - 1, here, c).wait_recv()
                    here[...] = (here[...].astype(jnp.float32) + term).astype(jnp.bfloat16)

                @pl.when(jnp.logical_not(arrives))
                def _():
                    here[...] = term.astype(jnp.bfloat16)

                sum_copy(d, t, here, c).start()
        attend(block(half - 1 - t), 0)
        attend(block(t + 1 - half), 1)
        return 0

    lax.fori_loop(1, half, sum_step, 0)
    for c in range(CHUNKS):
        term = partial(0, c)
        for d in range(2):
            sum_copy(d, half - 1, acc.at[d, half - 1, c], c).wait_recv()
            term = term + acc[d, half - 1, c].astype(jnp.float32)
        out_ref[:, pl.ds(c * width, width)] = term.astype(jnp.bfloat16)

    cores_kv.wait_send()
    ring = {"tp": right}
    whole(mine, pair_send.at[0], pair_recv.at[0], ring).wait_send()
    whole(tok.at[pl.ds(0, n - 1)], ag_send.at[0], ag_recv.at[0, 0, 0], ring).wait_send()
    whole(first, rs_send.at[0], rs_recv.at[0, 0, 0], ring).wait_send()
    whole(acc.at[:, pl.ds(0, half - 1)], rs_send.at[1], rs_recv.at[0, 0, 0], ring).wait_send()


def layer(n, cores, tokens, w_query, w_key, w_value, w_out, doc_lengths):
    rows, depth = tokens.shape
    hd = w_query.shape[1]
    half = n // 2
    total = n * cores * rows
    longest = total // 4
    window = min(-(-(longest + rows) // 128) * 128, total)
    width = depth // CHUNKS
    spread = np.power(
        np.float32(10000.0), -(np.arange(hd // 2, dtype=np.float32) * np.float32(2.0 / hd))
    ).astype(np.float32)
    freq = jnp.asarray(np.concatenate([spread, spread])[None, :])
    anywhere = pl.BlockSpec(memory_space=pl.ANY)
    vmem = pl.BlockSpec(memory_space=pltpu.VMEM)
    bf16, f32, dma = jnp.bfloat16, jnp.float32, pltpu.SemaphoreType.DMA
    return pl.pallas_call(
        functools.partial(kernel, n, window),
        out_shape=jax.ShapeDtypeStruct((rows, depth), bf16),
        in_specs=[anywhere] * 5 + [pl.BlockSpec(memory_space=pltpu.SMEM), vmem],
        out_specs=vmem,
        scratch_shapes=[
            pltpu.VMEM((n, rows, depth), bf16),
            pltpu.VMEM((depth, hd), bf16),
            pltpu.VMEM((hd, depth), bf16),
            pltpu.VMEM((hd, depth), bf16),
            pltpu.VMEM((n, rows, hd), f32),
            pltpu.VMEM((n, rows, hd), f32),
            pltpu.VMEM((n, rows, hd), bf16),
            pltpu.VMEM((n, rows, hd), bf16),
            pltpu.VMEM((n, rows, hd), bf16),
            pltpu.VMEM((total, 2 * hd), bf16),
            pltpu.VMEM((2, rows, hd), bf16),
            pltpu.VMEM((CHUNKS, rows, width), bf16),
            pltpu.VMEM((2, half, CHUNKS, rows, width), bf16),
            dma((5,)),
            dma((1,)),
            dma((2, SLOTS, CHUNKS)),
            dma((1,)),
            dma((n,)),
            dma((1,)),
            dma((1,)),
            dma((2,)),
            dma((2, SLOTS, CHUNKS)),
        ],
        compiler_params=pltpu.CompilerParams(
            collective_id=0, has_side_effects=True, vmem_limit_bytes=60 * 1024 * 1024
        ),
    )(tokens, w_query, w_key.T, w_value.T, w_out, doc_lengths, freq)


def solution(mesh):
    placed = (
        P(("groups", "tp", "sp"), None),
        P(None, "tp"),
        P(None, "tp"),
        P(None, "tp"),
        P("tp", None),
        P("groups"),
    )
    return jax.shard_map(
        functools.partial(layer, mesh.shape["tp"], mesh.shape["sp"]),
        mesh=mesh,
        in_specs=placed,
        out_specs=P(("groups", "tp", "sp"), None),
        check_vma=False,
    )
```
